32 devices in a mesh: gx: 4 (over x, core), gy: 4 (over z), gz: 2 (over y).
Axes of the slice: x: 2, y: 2, z: 4, core: 2. Of those that a mesh axis runs over, the one named last changes fastest.
Arguments:
- orbitals: float32 [16, 48, 48, 256], P(None, 'gx', 'gy', 'gz'), may hold values from -6 to 6
- potential: float32 [48, 48, 256], P('gx', 'gy', 'gz'), may hold values from 0 to 2
Outputs:
- filtered: float32 [16, 48, 48, 256], P(None, 'gx', 'gy', 'gz')
The draws below stay inside these ranges and needn't reach their ends.
All inputs are finite; a program needn't handle non-finite values.
Results may differ from the reference program's by a relative error of at most 0.00002.
Values sent between devices are 32-bit elements; how exact they have to be, the bound alone decides.
No kernel may reach another device: no remote copies, remote signals or barrier semaphores. Data moves between devices by JAX's collectives and lax.ppermute only.
A program may use at most 64 MiB of HBM per device.

```python
import jax
import jax.numpy as jnp
from jax import lax

BANDS = 16
DEGREE = 2
NX = 48
NY = 48
NZ = 256


def level_of(key, dims, cuts, least, high):
    loudness = 1.0
    for axis_at, blocks in cuts:
        heights = jax.random.uniform(jax.random.fold_in(jax.random.fold_in(key, 6), axis_at), (blocks,), jnp.float32, least / len(cuts), high / len(cuts))
        loudness = loudness * jnp.repeat(jnp.exp(heights), dims[axis_at] // blocks).reshape((-1,) + (1,) * (len(dims) - 1 - axis_at))
    return loudness


def normal_values(stream_key, dims, scale, most, split=(), kind=jnp.bfloat16):
    level = level_of(stream_key, dims, split, -0.22, 0.18) if split else 1.0
    array = jax.random.normal(stream_key, dims, jnp.float32) * scale * level
    return jnp.minimum(jnp.maximum(array, -most), most).astype(kind)


def setup_inputs(seed: int = 0) -> dict:
    streams_of = jax.random.split(jax.random.key(seed), 3)
    return {
        "orbitals": normal_values(streams_of[0], (BANDS, NX, NY, NZ), 1.0, 6.0, ((1, 4), (2, 4), (3, 2)), jnp.float32),
        "potential": jnp.clip(2.0 * jax.random.uniform(streams_of[1], (NX, NY, NZ), jnp.float32) ** level_of(streams_of[1], (NX, NY, NZ), ((0, 4), (1, 4), (2, 2)), -0.2, 0.2), 0.0, 2.0),
    }


SECOND = (-5369.0 / 1800.0, 12.0 / 7.0, -15.0 / 56.0, 10.0 / 189.0, -1.0 / 112.0, 2.0 / 1925.0, -1.0 / 16632.0)
FIRST = (6.0 / 7.0, -15.0 / 56.0, 5.0 / 63.0, -1.0 / 56.0, 3.0 / 385.0, -1.0 / 792.0)
METRIC = ((1.0, 0.25, 0.15), (0.25, 1.0, 0.2), (0.15, 0.2, 1.0))
CENTER = 10.5
HALF_WIDTH = 9.5


def window(values, starts, lengths):
    leading = values.ndim - 3
    starts_full = (0,) * leading + tuple(starts)
    limits = tuple(values.shape[:leading]) + tuple(s + l for s, l in zip(starts, lengths))
    return lax.slice(values, starts_full, limits)


def apply_operator(padded, potential):
    lengths = [padded.shape[i + 1] - 12 for i in range(3)]
    centre = window(padded, (6, 6, 6), lengths)
    summed = METRIC[0][0] * 0.0 * centre
    for d in range(3):
        second = SECOND[0] * centre
        for k in range(1, 7):
            forward = [6, 6, 6]
            forward[d] += k
            backward = [6, 6, 6]
            backward[d] -= k
            second = second + SECOND[k] * (window(padded, forward, lengths) + window(padded, backward, lengths))
        summed = summed + METRIC[d][d] * second
    for d, e in ((0, 1), (0, 2), (1, 2)):
        widened = list(lengths)
        widened[d] += 12
        partial_sum = None
        for k in range(1, 7):
            forward = [6, 6, 6]
            forward[d] = 0
            forward[e] += k
            backward = [6, 6, 6]
            backward[d] = 0
            backward[e] -= k
            term = FIRST[k - 1] * (window(padded, forward, widened) - window(padded, backward, widened))
            partial_sum = term if partial_sum is None else partial_sum + term
        crossed = None
        for k in range(1, 7):
            forward = [0, 0, 0]
            forward[d] = 6 + k
            backward = [0, 0, 0]
            backward[d] = 6 - k
            term = FIRST[k - 1] * (window(partial_sum, forward, lengths) - window(partial_sum, backward, lengths))
            crossed = term if crossed is None else crossed + term
        summed = summed + 2.0 * METRIC[d][e] * crossed
    return -0.5 * summed + potential[None] * centre


def reference(orbitals, potential):
    previous = jnp.zeros_like(orbitals)
    current = orbitals
    for degree_step in range(DEGREE):
        padded = jnp.pad(current, ((0, 0), (6, 6), (6, 6), (6, 6)), mode="wrap")
        applied = apply_operator(padded, potential)
        factor = 1.0 if degree_step == 0 else 2.0
        carry_factor = 0.0 if degree_step == 0 else 1.0
        following = factor * (applied - CENTER * current) / HALF_WIDTH - carry_factor * previous
        previous = current
        current = following
    return current
```

```python
import functools

import jax
import jax.numpy as jnp
import numpy as np
from jax import lax
from jax.experimental import pallas as pl
from jax.experimental.pallas import tpu as pltpu
from jax.sharding import PartitionSpec as P

DEGREE = 2
SECOND = (
    -5369.0 / 1800.0,
    12.0 / 7.0,
    -15.0 / 56.0,
    10.0 / 189.0,
    -1.0 / 112.0,
    2.0 / 1925.0,
    -1.0 / 16632.0,
)
FIRST = (6.0 / 7.0, -15.0 / 56.0, 5.0 / 63.0, -1.0 / 56.0, 3.0 / 385.0, -1.0 / 792.0)
METRIC = ((1.0, 0.25, 0.15), (0.25, 1.0, 0.2), (0.15, 0.2, 1.0))
CENTER = 10.5
HALF_WIDTH = 9.5
REACH = 6
SUB = 8
HIGHEST = lax.Precision.HIGHEST


def along_lanes(lanes):
    full = np.zeros((lanes + 2 * REACH, 2 * lanes), np.float64)
    for j in range(lanes):
        full[j + REACH, lanes + j] += METRIC[2][2] * SECOND[0]
        for k in range(1, REACH + 1):
            full[j + REACH + k, j] += FIRST[k - 1]
            full[j + REACH - k, j] -= FIRST[k - 1]
            full[j + REACH + k, lanes + j] += METRIC[2][2] * SECOND[k]
            full[j + REACH - k, lanes + j] += METRIC[2][2] * SECOND[k]
    inner = full[REACH : REACH + lanes]
    outer = np.zeros((2 * SUB, 2 * lanes), np.float64)
    outer[:REACH] = full[:REACH]
    outer[SUB : SUB + REACH] = full[REACH + lanes :]
    pick = np.zeros((2 * SUB, lanes), np.float64)
    for i in range(REACH):
        pick[i, i] = 1.0
        pick[SUB + i, lanes - REACH + i] = 1.0
    return tuple(m.astype(np.float32) for m in (inner, outer, pick))


def call(kernel, shapes, scratch=(), flops=0):
    return pl.pallas_call(
        kernel,
        out_shape=tuple(jax.ShapeDtypeStruct(s, jnp.float32) for s in shapes),
        scratch_shapes=[pltpu.VMEM(s, jnp.float32) for s in scratch],
        compiler_params=pltpu.CompilerParams(vmem_limit_bytes=48 * 1024 * 1024),
        cost_estimate=pl.CostEstimate(flops=flops, bytes_accessed=0, transcendentals=0),
    )


def pack_kernel(count, part, x_ref, o_ref):
    ways = SUB // part

    def row(y, _):
        for g in range(count):
            for w in range(ways):
                o_ref[g, y, :, w * part : (w + 1) * part, :] = x_ref[
                    :, w, y, g * part : (g + 1) * part, :
                ]
        return _

    lax.fori_loop(0, o_ref.shape[1], row, 0)


def unpack_kernel(count, part, x_ref, o_ref):
    ways = SUB // part

    def row(y, _):
        for g in range(count):
            for w in range(ways):
                o_ref[:, w, y, g * part : (g + 1) * part, :] = x_ref[
                    g, y, :, w * part : (w + 1) * part, :
                ]
        return _

    lax.fori_loop(0, x_ref.shape[1], row, 0)


def edges(ref, at, pick, low_ref, high_ref):
    rows = ref.shape[0] * ref.shape[1] * ref.shape[2] if len(ref.shape) == 4 else None
    v = ref[...].reshape(rows, ref.shape[-1])
    got = lax.dot_general(
        pick, v, (((1,), (1,)), ((), ())), precision=HIGHEST, preferred_element_type=jnp.float32
    )
    low_ref[:, at * rows : (at + 1) * rows] = got[:SUB]
    high_ref[:, at * rows : (at + 1) * rows] = got[SUB:]


def arrange_kernel(count, part, x_ref, pick_ref, a_ref, b_ref, low_ref, high_ref):
    ways = SUB // part
    groups = count // ways
    pairs = x_ref.shape[2]

    def row(y, _):
        for half, out in enumerate((a_ref, b_ref)):
            for g in range(count):
                h, q = divmod(g, groups)
                for k in range(pairs):
                    for w in range(ways):
                        out[y, (q * pairs + k) * ways + w, h * part : (h + 1) * part, :] = x_ref[
                            g, y + half * REACH, k, w * part : (w + 1) * part, :
                        ]
        return _

    lax.fori_loop(0, REACH, row, 0)
    pick = pick_ref[...]
    edges(a_ref, 0, pick, low_ref, high_ref)
    edges(b_ref, 1, pick, low_ref, high_ref)


def first_of(at):
    total = None
    for k in range(1, REACH + 1):
        term = FIRST[k - 1] * (at(k) - at(-k))
        total = term if total is None else total + term
    return total


def second_of(at):
    total = SECOND[0] * at(0)
    for k in range(1, REACH + 1):
        total = total + SECOND[k] * (at(k) + at(-k))
    return total


def step_kernel(count, part, scale, carry, last, *refs):
    pieces = refs[:4]
    halos = refs[4:8]
    pot_ref, inner_ref, outer_ref = refs[8:11]
    rest = refs[11:]
    if carry:
        befores, rest = rest[:2], rest[2:]
    if last:
        out_ref, d_ref, c_ref, w_ref = rest
    else:
        pick_ref, a_ref, b_ref, low_ref, high_ref, d_ref, c_ref, w_ref = rest
    xs = pieces[0].shape[1]
    lanes = pieces[0].shape[3]
    ways = SUB // part
    groups = count // ways

    inner = inner_ref[...]
    outer = outer_ref[...]
    for i in range(4):
        rows = REACH * xs * SUB
        z = lax.dot_general(
            pieces[i][...].reshape(rows, lanes),
            inner,
            (((1,), (0,)), ((), ())),
            precision=HIGHEST,
            preferred_element_type=jnp.float32,
        ) + lax.dot_general(
            halos[i][...],
            outer,
            (((0,), (0,)), ((), ())),
            precision=HIGHEST,
            preferred_element_type=jnp.float32,
        )
        d_ref[i * REACH : (i + 1) * REACH] = z[:, :lanes].reshape(REACH, xs, SUB, lanes)
        if i in (1, 2):
            c_ref[(i - 1) * REACH : i * REACH] = z[:, lanes:].reshape(REACH, xs, SUB, lanes)

    def column(x, _):
        v = [pieces[y // REACH][y % REACH, x] for y in range(4 * REACH)]
        for y in range(2 * REACH):
            w_ref[y, x] = (2.0 * METRIC[0][1]) * first_of(lambda k: v[y + REACH + k]) + (
                2.0 * METRIC[0][2]
            ) * d_ref[y + REACH, x]
        for y in range(2 * REACH):
            c_ref[y, x] = c_ref[y, x] + METRIC[1][1] * second_of(lambda k: v[y + REACH + k])
        d = [d_ref[y, x] for y in range(4 * REACH)]
        for y in range(2 * REACH):
            c_ref[y, x] = c_ref[y, x] + (2.0 * METRIC[1][2]) * first_of(lambda k: d[y + REACH + k])
        return _

    lax.fori_loop(0, xs, column, 0)

    def wrapped(values):
        def at(x):
            if x < 0:
                return pltpu.roll(values(x + xs), part, 0)
            if x >= xs:
                return pltpu.roll(values(x - xs), SUB - part, 0)
            return values(x)

        table = [at(x) for x in range(-REACH, xs + REACH)]
        return lambda x: table[x + REACH]

    def row(half, y, _):
        yy = half * REACH + y
        v = wrapped(lambda x: pieces[1 + half][y, x])
        w = wrapped(lambda x: w_ref[yy, x])
        for x in range(xs):
            total = (
                c_ref[yy, x]
                + METRIC[0][0] * second_of(lambda k: v(x + k))
                + first_of(lambda k: w(x + k))
            )
            value = (-0.5 * scale) * total + (scale * (pot_ref[yy, x] - CENTER)) * v(x)
            if carry:
                value = value - befores[half][y, x]
            if last:
                k, par = divmod(x, ways)
                q, k = divmod(k, xs // ways // groups)
                for h in range(ways):
                    out_ref[h * groups + q, yy, k, par * part : (par + 1) * part, :] = value[
                        h * part : (h + 1) * part
                    ]
            else:
                (a_ref, b_ref)[half][y, x] = value
        return _

    for half in range(2):
        lax.fori_loop(0, REACH, functools.partial(row, half), 0)
    if not last:
        pick = pick_ref[...]
        edges(a_ref, 0, pick, low_ref, high_ref)
        edges(b_ref, 1, pick, low_ref, high_ref)


def shift(value, axis, by):
    size = lax.axis_size(axis)
    return lax.ppermute(value, axis, [(i, (i + by) % size) for i in range(size)])


def local(orbitals, potential):
    bands, nx, ny, lanes = orbitals.shape
    count = lax.axis_size("gx")
    part = bands // count
    ways = SUB // part
    pairs = nx // ways
    xs = count * nx // ways
    assert ny == 2 * REACH and SUB % part == 0 and nx % ways == 0 and count % ways == 0
    rows = REACH * xs * SUB
    inner, outer, pick = along_lanes(lanes)

    native = jnp.transpose(orbitals, (1, 2, 0, 3)).reshape(pairs, ways, ny, bands, lanes)
    chunked = (count, ny, pairs, SUB, lanes)
    (packed,) = call(functools.partial(pack_kernel, count, part), [chunked])(native)
    swapped = lax.all_to_all(packed, "gx", split_axis=0, concat_axis=0, tiled=True)

    plane = lax.all_gather(jnp.transpose(potential, (1, 0, 2)), "gx", axis=1, tiled=True)
    plane = jnp.transpose(plane.reshape(ny, ways, xs, lanes), (0, 2, 1, 3))
    plane = jnp.broadcast_to(plane[:, :, :, None], (ny, xs, ways, part, lanes))
    plane = plane.reshape(ny, xs, SUB, lanes)

    piece = (REACH, xs, SUB, lanes)
    edge = (SUB, 2 * rows)
    a, b, low, high = call(
        functools.partial(arrange_kernel, count, part), [piece, piece, edge, edge], flops=40_000_000
    )(swapped, pick)
    before = None
    for step in range(DEGREE):
        last = step == DEGREE - 1
        from_low = shift(high, "gz", 1)
        from_high = shift(low, "gz", -1)
        b_down = shift(b, "gy", 1)
        a_up = shift(a, "gy", -1)
        halo_a = jnp.concatenate([from_low[:, :rows], from_high[:, :rows]], axis=0)
        halo_b = jnp.concatenate([from_low[:, rows:], from_high[:, rows:]], axis=0)
        halo_down = shift(halo_b, "gy", 1)
        halo_up = shift(halo_a, "gy", -1)
        scale = (1.0 if step == 0 else 2.0) / HALF_WIDTH
        arguments = [b_down, a, b, a_up, halo_down, halo_a, halo_b, halo_up, plane, inner, outer]
        if step:
            arguments += list(before)
        if not last:
            arguments.append(pick)
        outs = call(
            functools.partial(step_kernel, count, part, scale, step > 0, last),
            [chunked] if last else [piece, piece, edge, edge],
            [(4 * REACH, xs, SUB, lanes)] + [(2 * REACH, xs, SUB, lanes)] * 2,
            flops=400_000_000,
        )(*arguments)
        before = (a, b)
        if not last:
            a, b, low, high = outs
    back = lax.all_to_all(outs[0], "gx", split_axis=0, concat_axis=0, tiled=True)
    (native,) = call(
        functools.partial(unpack_kernel, count, part), [(pairs, ways, ny, bands, lanes)]
    )(back)
    return jnp.transpose(native.reshape(nx, ny, bands, lanes), (2, 0, 1, 3))


def solution(mesh):
    return jax.shard_map(
        local,
        mesh=mesh,
        in_specs=(P(None, "gx", "gy", "gz"), P("gx", "gy", "gz")),
        out_specs=P(None, "gx", "gy", "gz"),
        check_vma=False,
    )
```

```python
import functools

import jax
import jax.numpy as jnp
import numpy as np
from jax import lax
from jax.experimental import pallas as pl
from jax.experimental.pallas import tpu as pltpu
from jax.sharding import PartitionSpec as P

DEGREE = 2
SECOND = (
    -5369.0 / 1800.0,
    12.0 / 7.0,
    -15.0 / 56.0,
    10.0 / 189.0,
    -1.0 / 112.0,
    2.0 / 1925.0,
    -1.0 / 16632.0,
)
FIRST = (6.0 / 7.0, -15.0 / 56.0, 5.0 / 63.0, -1.0 / 56.0, 3.0 / 385.0, -1.0 / 792.0)
METRIC = ((1.0, 0.25, 0.15), (0.25, 1.0, 0.2), (0.15, 0.2, 1.0))
CENTER = 10.5
HALF_WIDTH = 9.5
REACH = 6
SUB = 8


def along_lanes(lanes):
    full = np.zeros((lanes + 2 * REACH, 2 * lanes), np.float64)
    for j in range(lanes):
        full[j + REACH, lanes + j] += METRIC[2][2] * SECOND[0]
        for k in range(1, REACH + 1):
            full[j + REACH + k, j] += FIRST[k - 1]
            full[j + REACH - k, j] -= FIRST[k - 1]
            full[j + REACH + k, lanes + j] += METRIC[2][2] * SECOND[k]
            full[j + REACH - k, lanes + j] += METRIC[2][2] * SECOND[k]
    inner = full[REACH : REACH + lanes]
    outer = np.zeros((2 * SUB, 2 * lanes), np.float64)
    outer[:REACH] = full[:REACH]
    outer[SUB : SUB + REACH] = full[REACH + lanes :]
    pick = np.zeros((2 * SUB, lanes), np.float64)
    for i in range(REACH):
        pick[i, i] = 1.0
        pick[SUB + i, lanes - REACH + i] = 1.0
    inner_high, inner_low = halves_of(inner)
    outer_high, outer_low = halves_of(outer)
    inner = np.block([[inner_high, inner_low], [inner_high, inner_low]])
    outer = np.concatenate([outer_high, outer_low, outer_high, outer_low], axis=0)
    pick = np.concatenate([pick, pick], axis=1)
    return tuple(m.astype(jnp.bfloat16) for m in (inner, outer, pick))


def halves_of(matrix):
    high = matrix.astype(jnp.bfloat16).astype(np.float64)
    return high, (matrix - high).astype(jnp.bfloat16).astype(np.float64)


def split(v):
    high = v.astype(jnp.bfloat16)
    return high, (v - high.astype(jnp.float32)).astype(jnp.bfloat16)


def product(left, right, left_dim, right_dim):
    return lax.dot_general(
        left, right, (((left_dim,), (right_dim,)), ((), ())), preferred_element_type=jnp.float32
    )


def call(kernel, shapes, scratch=(), flops=0, **more):
    return pl.pallas_call(
        kernel,
        **more,
        out_shape=tuple(jax.ShapeDtypeStruct(s, jnp.float32) for s in shapes),
        scratch_shapes=[pltpu.VMEM(s, jnp.float32) for s in scratch],
        compiler_params=pltpu.CompilerParams(vmem_limit_bytes=48 * 1024 * 1024),
        cost_estimate=pl.CostEstimate(flops=flops, bytes_accessed=0, transcendentals=0),
    )


def pack_kernel(x_ref, o_ref):
    count, rows = o_ref.shape[:2]
    for g in range(count):
        o_ref[g] = x_ref[pl.ds(g, rows, stride=count), :]


def unpack_kernel(x_ref, o_ref):
    count, rows = x_ref.shape[:2]
    for g in range(count):
        o_ref[pl.ds(g, rows, stride=count), :] = x_ref[g]


def spots(counts, nx, ny):
    xs = nx * counts[0] // SUB
    for gx in range(counts[0]):
        for gy in range(counts[1]):
            for x in range(nx):
                h, at = divmod(gx * nx + x, xs)
                yield gx * counts[1] + gy, x * ny, pl.ds((gy * ny * xs + at) * SUB + h, ny, stride=xs * SUB)


def arrange_kernel(counts, nx, ny, x_ref, o_ref):
    for g, start, rows in spots(counts, nx, ny):
        o_ref[rows, :] = x_ref[g, start : start + ny, :]


def plane_kernel(counts, nx, ny, place_ref, x_ref, o_ref):
    for g, start, rows in spots(counts, nx, ny):
        gx, gy = divmod(g, counts[1])
        back_x = lax.rem(place_ref[0] + (counts[0] - gx), counts[0])
        back_y = lax.rem(place_ref[1] + (counts[1] - gy), counts[1])
        o_ref[rows, :] = x_ref[back_x, back_y, start : start + ny, :]


def scatter_kernel(counts, nx, ny, x_ref, o_ref):
    for g, start, rows in spots(counts, nx, ny):
        o_ref[g, start : start + ny, :] = x_ref[rows, :]


def edges(ref, pick_ref, low_ref, high_ref):
    got = product(pick_ref[...], jnp.concatenate(split(ref[...]), axis=1), 1, 1)
    low_ref[...] = got[:SUB]
    high_ref[...] = got[SUB:]


def begin_kernel(counts, nx, ny, x_ref, pick_ref, o_ref, low_ref, high_ref):
    arrange_kernel(counts, nx, ny, x_ref, o_ref)
    edges(o_ref, pick_ref, low_ref, high_ref)


def first_of(at):
    total = None
    for k in range(1, REACH + 1):
        term = FIRST[k - 1] * (at(k) - at(-k))
        total = term if total is None else total + term
    return total


def second_of(at):
    total = SECOND[0] * at(0)
    for k in range(1, REACH + 1):
        total = total + SECOND[k] * (at(k) + at(-k))
    return total


def step_kernel(counts, nx, ny, scale, carry, last, *refs):
    v_ref, from_low, from_high, pot_ref, inner_ref, outer_ref = refs[:6]
    rest = refs[6:]
    if carry:
        before_ref, rest = rest[0], rest[1:]
    if last:
        spread_ref, d_ref, c_ref, w_ref, out_ref = rest
    else:
        pick_ref, out_ref, low_ref, high_ref, d_ref, c_ref, w_ref = rest
    lanes = v_ref.shape[1]
    xs = nx * counts[0] // SUB
    ys = ny * counts[1]
    chunk = REACH * 2

    def at(y, x):
        return pl.ds(pl.multiple_of((y * xs + x) * SUB, SUB), SUB), slice(None)

    inner = inner_ref[...]
    outer = outer_ref[...]
    size = v_ref.shape[0] // 2
    for i in range(2):
        part = slice(i * size, (i + 1) * size)
        v = jnp.concatenate(split(v_ref[part, :]), axis=1)
        wide = product(v, inner, 1, 0)
        z = wide[:, : 2 * lanes] + wide[:, 2 * lanes :]
        high, low = split(jnp.concatenate([from_low[:, part], from_high[:, part]], axis=0))
        z = z + product(jnp.concatenate([high, high, low, low], axis=0), outer, 0, 0)
        d_ref[part, :] = z[:, :lanes]
        c_ref[part, :] = z[:, lanes:]

    for first in range(0, ys, chunk):

        def column(x, _):
            v = [v_ref[at((first + y) % ys, x)] for y in range(-REACH, chunk + REACH)]
            for y in range(chunk):
                w_ref[at(first + y, x)] = (2.0 * METRIC[0][1]) * first_of(
                    lambda k: v[y + REACH + k]
                ) + (2.0 * METRIC[0][2]) * d_ref[at(first + y, x)]
            for y in range(chunk):
                here = at(first + y, x)
                c_ref[here] = c_ref[here] + METRIC[1][1] * second_of(lambda k: v[y + REACH + k])
            d = [d_ref[at((first + y) % ys, x)] for y in range(-REACH, chunk + REACH)]
            for y in range(chunk):
                here = at(first + y, x)
                c_ref[here] = c_ref[here] + (2.0 * METRIC[1][2]) * first_of(
                    lambda k: d[y + REACH + k]
                )
            return _

        lax.fori_loop(0, xs, column, 0)

    def wrapped(ref, y):
        values = [ref[at(y, x)] for x in range(xs)]

        def one(x):
            turns, x = divmod(x, xs)
            value = values[x]
            return pltpu.roll(value, -turns % SUB, 0) if turns else value

        table = [one(x) for x in range(-REACH, xs + REACH)]
        return lambda x: table[x + REACH]

    def row(y, _):
        v = wrapped(v_ref, y)
        w = wrapped(w_ref, y)
        for x in range(xs):
            here = at(y, x)
            total = (
                c_ref[here]
                + METRIC[0][0] * second_of(lambda k: v(x + k))
                + first_of(lambda k: w(x + k))
            )
            value = (-0.5 * scale) * total + (scale * (pot_ref[here] - CENTER)) * v(x)
            if carry:
                value = value - before_ref[here]
            out_ref[here] = value
        return _

    lax.fori_loop(0, ys, row, 0)
    if last:
        scatter_kernel(counts, nx, ny, out_ref, spread_ref)
    else:
        edges(out_ref, pick_ref, low_ref, high_ref)


def shift(value, axis, by):
    size = lax.axis_size(axis)
    return lax.ppermute(value, axis, [(i, (i + by) % size) for i in range(size)])


def local(orbitals, potential):
    bands, nx, ny, lanes = orbitals.shape
    axes = ("gx", "gy")
    counts = tuple(lax.axis_size(axis) for axis in axes)
    count = counts[0] * counts[1]
    rows = count * nx * ny
    assert bands == count and nx * counts[0] % SUB == 0 and nx * counts[0] // SUB >= 1
    assert ny * counts[1] % (2 * REACH) == 0 and rows % 256 == 0
    inner, outer, pick = along_lanes(lanes)
    sizes = (counts, nx, ny)

    native = jnp.transpose(orbitals, (1, 2, 0, 3)).reshape(nx * ny * bands, lanes)
    chunked = (count, nx * ny, lanes)
    whole = (rows, lanes)
    edge = (SUB, rows)
    own = potential.reshape(nx * ny, lanes)
    column = jnp.stack([own] + [shift(own, "gy", k) for k in range(1, counts[1])])
    (packed,) = call(pack_kernel, [chunked])(native)
    packed, column = lax.optimization_barrier((packed, column))
    gathered = jnp.stack([column] + [shift(column, "gx", k) for k in range(1, counts[0])])
    place = jnp.stack([lax.axis_index(axis) for axis in axes]).astype(jnp.int32)
    swapped = lax.all_to_all(packed, axes, split_axis=0, concat_axis=0, tiled=True)
    current, low, high = call(
        functools.partial(begin_kernel, *sizes), [whole, edge, edge], flops=20_000_000
    )(swapped, pick)
    (plane,) = call(
        functools.partial(plane_kernel, *sizes),
        [whole],
        flops=10_000_000,
        in_specs=[
            pl.BlockSpec(memory_space=pltpu.SMEM),
            pl.BlockSpec(memory_space=pltpu.VMEM),
        ],
    )(place, gathered)
    before = None
    for step in range(DEGREE):
        last = step == DEGREE - 1
        scale = (1.0 if step == 0 else 2.0) / HALF_WIDTH
        arguments = [current, shift(high, "gz", 1), shift(low, "gz", -1), plane, inner, outer]
        if step:
            arguments.append(before)
        if not last:
            arguments.append(pick)
        outs = call(
            functools.partial(step_kernel, *sizes, scale, step > 0, last),
            [chunked] if last else [whole, edge, edge],
            [whole] * (4 if last else 3),
            flops=100_000_000,
        )(*arguments)
        before = current
        if not last:
            current, low, high = outs
    back = lax.all_to_all(outs[0], axes, split_axis=0, concat_axis=0, tiled=True)
    (native,) = call(unpack_kernel, [(nx * ny * bands, lanes)])(back)
    return jnp.transpose(native.reshape(nx, ny, bands, lanes), (2, 0, 1, 3))


def solution(mesh):
    return jax.shard_map(
        local,
        mesh=mesh,
        in_specs=(P(None, "gx", "gy", "gz"), P("gx", "gy", "gz")),
        out_specs=P(None, "gx", "gy", "gz"),
        check_vma=False,
    )
```

```python
import functools

import jax
import jax.numpy as jnp
import numpy as np
from jax import lax
from jax.experimental import pallas as pl
from jax.experimental.pallas import tpu as pltpu
from jax.sharding import PartitionSpec as P

DEGREE = 2
SECOND = (
    -5369.0 / 1800.0,
    12.0 / 7.0,
    -15.0 / 56.0,
    10.0 / 189.0,
    -1.0 / 112.0,
    2.0 / 1925.0,
    -1.0 / 16632.0,
)
FIRST = (6.0 / 7.0, -15.0 / 56.0, 5.0 / 63.0, -1.0 / 56.0, 3.0 / 385.0, -1.0 / 792.0)
METRIC = ((1.0, 0.25, 0.15), (0.25, 1.0, 0.2), (0.15, 0.2, 1.0))
CENTER = 10.5
HALF_WIDTH = 9.5
REACH = 6
SUB = 8


def along_lanes(lanes):
    full = np.zeros((lanes + 2 * REACH, 2 * lanes), np.float64)
    for j in range(lanes):
        full[j + REACH, lanes + j] += METRIC[2][2] * SECOND[0]
        for k in range(1, REACH + 1):
            full[j + REACH + k, j] += FIRST[k - 1]
            full[j + REACH - k, j] -= FIRST[k - 1]
            full[j + REACH + k, lanes + j] += METRIC[2][2] * SECOND[k]
            full[j + REACH - k, lanes + j] += METRIC[2][2] * SECOND[k]
    inner = full[REACH : REACH + lanes]
    outer = np.zeros((2 * SUB, 2 * lanes), np.float64)
    outer[:REACH] = full[:REACH]
    outer[SUB : SUB + REACH] = full[REACH + lanes :]
    pick = np.zeros((2 * SUB, lanes), np.float64)
    for i in range(REACH):
        pick[i, i] = 1.0
        pick[SUB + i, lanes - REACH + i] = 1.0
    inner_high, inner_low = halves_of(inner)
    outer_high, outer_low = halves_of(outer)
    inner = np.block([[inner_high, inner_low], [inner_high, inner_low]])
    outer = np.concatenate([outer_high, outer_low, outer_high, outer_low], axis=0)
    pick = np.concatenate([pick, pick], axis=1)
    return tuple(m.astype(jnp.bfloat16) for m in (inner, outer, pick))


def halves_of(matrix):
    high = matrix.astype(jnp.bfloat16).astype(np.float64)
    return high, (matrix - high).astype(jnp.bfloat16).astype(np.float64)


def split(v):
    high = v.astype(jnp.bfloat16)
    return high, (v - high.astype(jnp.float32)).astype(jnp.bfloat16)


def product(left, right, left_dim, right_dim):
    return lax.dot_general(
        left, right, (((left_dim,), (right_dim,)), ((), ())), preferred_element_type=jnp.float32
    )


def call(kernel, shapes, scratch=(), flops=0, **more):
    return pl.pallas_call(
        kernel,
        **more,
        out_shape=tuple(jax.ShapeDtypeStruct(s, jnp.float32) for s in shapes),
        scratch_shapes=[pltpu.VMEM(s, jnp.float32) for s in scratch],
        compiler_params=pltpu.CompilerParams(vmem_limit_bytes=48 * 1024 * 1024),
        cost_estimate=pl.CostEstimate(flops=flops, bytes_accessed=0, transcendentals=0),
    )


def pack_kernel(x_ref, o_ref):
    count, rows = o_ref.shape[:2]
    for g in range(count):
        o_ref[g] = x_ref[pl.ds(g, rows, stride=count), :]


def unpack_kernel(x_ref, o_ref):
    count, rows = x_ref.shape[:2]
    for g in range(count):
        o_ref[pl.ds(g, rows, stride=count), :] = x_ref[g]


def spots(counts, nx, ny):
    xs = nx * counts[0] // SUB
    for gx in range(counts[0]):
        for gy in range(counts[1]):
            for x in range(nx):
                h, at = divmod(gx * nx + x, xs)
                yield gx * counts[1] + gy, x * ny, pl.ds((gy * ny * xs + at) * SUB + h, ny, stride=xs * SUB)


def arrange_kernel(counts, nx, ny, x_ref, o_ref):
    for g, start, rows in spots(counts, nx, ny):
        o_ref[rows, :] = x_ref[g, start : start + ny, :]


def plane_kernel(counts, nx, ny, place_ref, x_ref, o_ref):
    for g, start, rows in spots(counts, nx, ny):
        gx, gy = divmod(g, counts[1])
        back_x = lax.rem(place_ref[0] + (counts[0] - gx), counts[0])
        back_y = lax.rem(place_ref[1] + (counts[1] - gy), counts[1])
        o_ref[rows, :] = x_ref[back_x, back_y, start : start + ny, :]


def scatter_kernel(counts, nx, ny, x_ref, o_ref):
    for g, start, rows in spots(counts, nx, ny):
        o_ref[g, start : start + ny, :] = x_ref[rows, :]


def edges(ref, pick_ref, low_ref, high_ref):
    got = product(pick_ref[...], jnp.concatenate(split(ref[...]), axis=1), 1, 1)
    low_ref[...] = got[:SUB]
    high_ref[...] = got[SUB:]


def begin_kernel(counts, nx, ny, x_ref, pick_ref, o_ref, low_ref, high_ref):
    arrange_kernel(counts, nx, ny, x_ref, o_ref)
    edges(o_ref, pick_ref, low_ref, high_ref)


def first_of(at):
    total = None
    for k in range(1, REACH + 1):
        term = FIRST[k - 1] * (at(k) - at(-k))
        total = term if total is None else total + term
    return total


def second_of(at):
    total = SECOND[0] * at(0)
    for k in range(1, REACH + 1):
        total = total + SECOND[k] * (at(k) + at(-k))
    return total


def step_kernel(counts, nx, ny, scale, carry, last, *refs):
    v_ref, from_low, from_high, pot_ref, inner_ref, outer_ref = refs[:6]
    rest = refs[6:]
    if carry:
        before_ref, rest = rest[0], rest[1:]
    if last:
        spread_ref, d_ref, c_ref, w_ref, out_ref = rest
    else:
        pick_ref, out_ref, low_ref, high_ref, d_ref, c_ref, w_ref = rest
    lanes = v_ref.shape[1]
    xs = nx * counts[0] // SUB
    ys = ny * counts[1]
    chunk = REACH * 2

    def at(y, x):
        return pl.ds(pl.multiple_of((y * xs + x) * SUB, SUB), SUB), slice(None)

    inner = inner_ref[...]
    outer = outer_ref[...]
    size = v_ref.shape[0] // 2
    for i in range(2):
        part = slice(i * size, (i + 1) * size)
        v = jnp.concatenate(split(v_ref[part, :]), axis=1)
        wide = product(v, inner, 1, 0)
        z = wide[:, : 2 * lanes] + wide[:, 2 * lanes :]
        high, low = split(jnp.concatenate([from_low[:, part], from_high[:, part]], axis=0))
        z = z + product(jnp.concatenate([high, high, low, low], axis=0), outer, 0, 0)
        d_ref[part, :] = z[:, :lanes]
        c_ref[part, :] = z[:, lanes:]

    for first in range(0, ys, chunk):

        def column(x, _):
            v = [v_ref[at((first + y) % ys, x)] for y in range(-REACH, chunk + REACH)]
            for y in range(chunk):
                w_ref[at(first + y, x)] = (2.0 * METRIC[0][1]) * first_of(
                    lambda k: v[y + REACH + k]
                ) + (2.0 * METRIC[0][2]) * d_ref[at(first + y, x)]
            for y in range(chunk):
                here = at(first + y, x)
                c_ref[here] = c_ref[here] + METRIC[1][1] * second_of(lambda k: v[y + REACH + k])
            d = [d_ref[at((first + y) % ys, x)] for y in range(-REACH, chunk + REACH)]
            for y in range(chunk):
                here = at(first + y, x)
                c_ref[here] = c_ref[here] + (2.0 * METRIC[1][2]) * first_of(
                    lambda k: d[y + REACH + k]
                )
            return _

        lax.fori_loop(0, xs, column, 0)

    def wrapped(ref, y):
        values = [ref[at(y, x)] for x in range(xs)]

        def one(x):
            turns, x = divmod(x, xs)
            value = values[x]
            return pltpu.roll(value, -turns % SUB, 0) if turns else value

        table = [one(x) for x in range(-REACH, xs + REACH)]
        return lambda x: table[x + REACH]

    def row(y, _):
        v = wrapped(v_ref, y)
        w = wrapped(w_ref, y)
        for x in range(xs):
            here = at(y, x)
            total = (
                c_ref[here]
                + METRIC[0][0] * second_of(lambda k: v(x + k))
                + first_of(lambda k: w(x + k))
            )
            value = (-0.5 * scale) * total + (scale * (pot_ref[here] - CENTER)) * v(x)
            if carry:
                value = value - before_ref[here]
            out_ref[here] = value
        return _

    lax.fori_loop(0, ys, row, 0)
    if last:
        scatter_kernel(counts, nx, ny, out_ref, spread_ref)
    else:
        edges(out_ref, pick_ref, low_ref, high_ref)


def shift(value, axis, by):
    size = lax.axis_size(axis)
    return lax.ppermute(value, axis, [(i, (i + by) % size) for i in range(size)])


def local(orbitals, potential):
    bands, nx, ny, lanes = orbitals.shape
    axes = ("gx", "gy")
    counts = tuple(lax.axis_size(axis) for axis in axes)
    count = counts[0] * counts[1]
    rows = count * nx * ny
    assert bands == count and nx * counts[0] % SUB == 0 and nx * counts[0] // SUB >= 1
    assert ny * counts[1] % (2 * REACH) == 0 and rows % 256 == 0
    inner, outer, pick = along_lanes(lanes)
    sizes = (counts, nx, ny)

    native = jnp.transpose(orbitals, (1, 2, 0, 3)).reshape(nx * ny * bands, lanes)
    chunked = (count, nx * ny, lanes)
    whole = (rows, lanes)
    edge = (SUB, rows)
    own = potential.reshape(nx * ny, lanes)
    stripes = [own] + [shift(own, "gy", k) for k in range(1, counts[1])]
    (packed,) = call(pack_kernel, [chunked], flops=20_000_000)(native)
    packed, *stripes = lax.optimization_barrier((packed, *stripes))
    column = jnp.stack(stripes)
    gathered = jnp.stack([column] + [shift(column, "gx", k) for k in range(1, counts[0])])
    place = jnp.stack([lax.axis_index(axis) for axis in axes]).astype(jnp.int32)
    swapped = lax.all_to_all(packed, axes, split_axis=0, concat_axis=0, tiled=True)
    current, low, high = call(
        functools.partial(begin_kernel, *sizes), [whole, edge, edge], flops=20_000_000
    )(swapped, pick)
    (plane,) = call(
        functools.partial(plane_kernel, *sizes),
        [whole],
        flops=10_000_000,
        in_specs=[
            pl.BlockSpec(memory_space=pltpu.SMEM),
            pl.BlockSpec(memory_space=pltpu.VMEM),
        ],
    )(place, gathered)
    before = None
    for step in range(DEGREE):
        last = step == DEGREE - 1
        scale = (1.0 if step == 0 else 2.0) / HALF_WIDTH
        arguments = [current, shift(high, "gz", 1), shift(low, "gz", -1), plane, inner, outer]
        if step:
            arguments.append(before)
        if not last:
            arguments.append(pick)
        outs = call(
            functools.partial(step_kernel, *sizes, scale, step > 0, last),
            [chunked] if last else [whole, edge, edge],
            [whole] * (4 if last else 3),
            flops=100_000_000,
        )(*arguments)
        before = current
        if not last:
            current, low, high = outs
    back = lax.all_to_all(outs[0], axes, split_axis=0, concat_axis=0, tiled=True)
    (native,) = call(unpack_kernel, [(nx * ny * bands, lanes)])(back)
    return jnp.transpose(native.reshape(nx, ny, bands, lanes), (2, 0, 1, 3))


def solution(mesh):
    return jax.shard_map(
        local,
        mesh=mesh,
        in_specs=(P(None, "gx", "gy", "gz"), P("gx", "gy", "gz")),
        out_specs=P(None, "gx", "gy", "gz"),
        check_vma=False,
    )
```
